32 devices in a mesh: prow: 4 (over y, core), pcol: 8 (over z, x).
Axes of the slice: x: 2, y: 2, z: 4, core: 2. Of those that a mesh axis runs over, the one named last changes fastest.
Arguments:
- inverse_cov: bfloat16 [8192, 8192], P('prow', 'pcol'), may hold values from -0.5 to 4.5, as said below
- cosines: float32 [8192, 8192], P('prow', 'pcol'), may hold values from -1 to 1, as said below
- sky_maps: bfloat16 [8192, 192], P('pcol'), may hold values from -6 to 6
Outputs:
- filtered: bfloat16 [8192, 192], P('prow')
- spectra: float32 [64, 192], replicated
The draws below stay inside these ranges and needn't reach their ends.
Inputs may be any that keep to these rules, and one draw needn't show every extreme that they name: `inverse_cov`: symmetric, with a dominant diagonal. `cosines`: symmetric.
All inputs are finite; a program needn't handle non-finite values.
Results may differ from the reference program's by a relative error of at most 0.0033.
Values may be sent and summed in bfloat16 or wider, within the bound.
A program may use at most 128 MiB of HBM per device.

```python
import math
import jax
import jax.numpy as jnp
from jax import lax

NPIX = 8192
MAPS = 192
L = 64
LMIN = 2


def draw_inverse_cov(key, part):
    first_key, second_key = jax.random.split(jax.random.fold_in(key, 11))
    noise = jax.random.truncated_normal(first_key, -6.0, 6.0, (NPIX, NPIX), jnp.float32) * (0.5 / math.sqrt(NPIX))
    symmetric = noise + noise.T
    diagonal = jax.random.uniform(second_key, (NPIX,), jnp.float32, 1.0, 2.0)
    return (symmetric + jnp.diag(diagonal)).astype(jnp.bfloat16)


def draw_cosines(key, part):
    vector_key, rough_key = jax.random.split(jax.random.fold_in(key, 23))
    vectors = jax.random.normal(vector_key, (NPIX, 3), jnp.float32)
    rough = jax.random.truncated_normal(rough_key, -4.0, 4.0, (NPIX, NPIX), jnp.float32) * 0.05
    units = vectors / jnp.sqrt(jnp.sum(vectors * vectors, axis=1, keepdims=True) + 1e-12)
    product = jnp.dot(units, units.T, precision=lax.Precision.HIGHEST)
    return jnp.clip(product + rough + rough.T, -1.0, 1.0)


def shard_levels(rng, extent, pieces, smallest, high):
    level = 1.0
    for dim, shards_of in pieces:
        steps = jax.random.uniform(jax.random.fold_in(jax.random.fold_in(rng, 6), dim), (shards_of,), jnp.float32, smallest / len(pieces), high / len(pieces))
        level = level * jnp.repeat(jnp.exp(steps), extent[dim] // shards_of).reshape((-1,) + (1,) * (len(extent) - 1 - dim))
    return level


def normal_values(rng, shape, scale, limit, cuts=(), kind=jnp.bfloat16):
    values = scale * jax.random.normal(rng, shape, jnp.float32)
    if cuts:
        values = values * shard_levels(rng, shape, cuts, -0.22, 0.18)
    return jnp.clip(values, -limit, limit).astype(kind)


def setup_inputs(seed: int = 0) -> dict:
    streams_of = jax.random.split(jax.random.key(seed), 4)
    inverse_cov = draw_inverse_cov(jax.random.fold_in(streams_of[3], 71), 0)
    cosines = draw_cosines(jax.random.fold_in(streams_of[3], 71), 0)
    sky_maps = normal_values(streams_of[2], (NPIX, MAPS), 1.0, 6.0, ((0, 8),))
    return {"inverse_cov": inverse_cov, "cosines": cosines, "sky_maps": sky_maps}


def next_legendre(previous, current, cosine, degree):
    return ((2.0 * degree - 1.0) * cosine * current - (degree - 1.0) * previous) / degree


def reference(inverse_cov, cosines, sky_maps):
    filtered = jnp.dot(inverse_cov, sky_maps, preferred_element_type=jnp.float32).astype(jnp.bfloat16)
    maps_f32 = filtered.astype(jnp.float32)
    blocks = 8
    size_rows = NPIX // blocks
    degrees = (jnp.arange(L) + LMIN).astype(jnp.float32)

    def block_spectra(block_index):
        first_row = (block_index * size_rows).astype(jnp.int32)
        cosine = lax.dynamic_slice_in_dim(cosines, first_row, size_rows, 0)
        rows_f32 = lax.dynamic_slice_in_dim(maps_f32, first_row, size_rows, 0)
        previous = jnp.ones_like(cosine)
        current = cosine
        for low_degree in range(2, LMIN):
            next_term = next_legendre(previous, current, cosine, jnp.float32(low_degree))
            previous, current = current, next_term

        def advance(carried, degree):
            previous, current = carried
            next_term = next_legendre(previous, current, cosine, degree)
            product = jnp.dot(next_term.astype(jnp.bfloat16), filtered, preferred_element_type=jnp.float32)
            spectrum = jnp.sum(rows_f32 * product, axis=0) * ((2.0 * degree + 1.0) / NPIX)
            return (current, next_term), spectrum

        carried, values = lax.scan(advance, (previous, current), degrees)
        return values

    per_block = lax.map(block_spectra, jnp.arange(blocks, dtype=jnp.int32))
    return filtered, jnp.sum(per_block, axis=0)
```

```python
import functools
import math
import random

import jax
import jax.numpy as jnp
import numpy as np
from jax import lax
from jax.experimental import pallas as pl
from jax.experimental.pallas import tpu as pltpu
from jax.sharding import PartitionSpec as P

L = 64
LMIN = 2
TILE = 256
STRIP = 16
GROUP = 11
CHUNKS = 6
LEVELS = GROUP * CHUNKS


def transform_matrix(npix):
    top = LMIN + L - 1
    a = [math.comb(2 * k, k) / 4.0**k for k in range(top + 1)]
    out = np.zeros((L, LEVELS + 1))
    for l in range(LMIN, top + 1):
        for k in range(l + 1):
            degree = abs(l - 2 * k)
            column = degree - 1 if degree else LEVELS
            out[l - LMIN, column] += a[k] * a[l - k]
        out[l - LMIN] *= (2 * l + 1) / npix
    return out.astype(np.float32)


def pair_up(tiles, n):
    items = []
    for col in range(n):
        mine = sorted((t for t in tiles if t[1] == col), key=lambda t: t[0])
        for k in range(0, len(mine), 2):
            first = mine[k]
            second = mine[k + 1] if k + 1 < len(mine) else (first[0], col, 0)
            items.append((first[0], second[0], first[2], second[2], col))
    return items


def work_tables(n):
    lower = [[(h * n + i, j, 2) for i in range(n) for j in range(n)] for h in range(2)]
    rng = random.Random(0)
    best = None
    for _ in range(20000):
        sets = []
        cross = [[rng.random() < 0.5 for _ in range(n)] for _ in range(n)]
        for h in range(2):
            tiles = []
            for i in range(n):
                tiles.append((h * n + i, i, 1))
                for j in range(i):
                    a, b = (i, j) if rng.random() < 0.5 else (j, i)
                    tiles.append((h * n + a, b, 2))
                for j in range(n):
                    if h == 0 and cross[i][j]:
                        tiles.append((n + i, j, 2))
                    if h == 1 and not cross[i][j]:
                        tiles.append((j, i, 2))
            sets.append(pair_up(tiles, n))
        cost = max(len(s) for s in sets)
        if best is None or cost < best[0]:
            best = (cost, sets)
        if 2 * cost <= n * n + n // 2 + 1:
            break
    kinds = [pair_up(lower[0], n), pair_up(lower[1], n), pair_up(lower[1], n), pair_up(lower[0], n)] + best[1]
    longest = max(len(k) for k in kinds)
    table = np.zeros((len(kinds), longest + 1, 5), np.int32)
    for k, items in enumerate(kinds):
        table[k, : len(items)] = items
    counts = np.array([len(k) for k in kinds], np.int32)
    return table.reshape(-1), counts, longest + 1


def moments_kernel(
    stride, table, counts, cos_hbm, ft, fct, out,
    xbuf, x2, prev, cur, buf_a, buf_b, lhs, fj, acc, sem,
):
    r = lax.axis_index("prow")
    c = lax.axis_index("pcol")
    q, h = c // 2, c % 2
    kind = jnp.where(r > q, h, jnp.where(r < q, 2 + h, 4 + h))
    n_items = counts[kind]

    def field(item, f):
        return table[(kind * stride + item) * 5 + f]

    def tile_copy(item, half):
        row = pl.multiple_of(field(item, half) * TILE, TILE)
        col = pl.multiple_of(field(item, 4) * TILE, TILE)
        return pltpu.make_async_copy(
            cos_hbm.at[pl.ds(row, TILE), pl.ds(col, TILE)],
            xbuf.at[pl.ds(half * TILE, TILE)],
            sem.at[half],
        )

    def fetch(item):
        tile_copy(item, 0).start()
        tile_copy(item, 1).start()

    def begin(item):
        tile_copy(item, 0).wait()
        tile_copy(item, 1).wait()
        x = xbuf[...]
        x2[...] = x + x
        prev[...] = x
        cur[...] = jnp.ones_like(x)

    def set_operands(item):
        col = pl.multiple_of(field(item, 4) * TILE, TILE)
        for half in range(2):
            row = pl.multiple_of(field(item, half) * TILE, TILE)
            weight = field(item, 2 + half).astype(jnp.float32)
            value = ft[:, pl.ds(row, TILE)].astype(jnp.float32) * weight
            lhs[:, half * TILE : (half + 1) * TILE] = value.astype(jnp.bfloat16)
        fj[...] = fct[:, pl.ds(col, TILE)].astype(jnp.float32)

    n_strips = 2 * TILE // STRIP

    def gen_strip(buf, s):
        rows = pl.ds(s * STRIP, STRIP)
        xx = x2[rows, :]
        p = prev[rows, :]
        t = cur[rows, :]
        for g in range(GROUP):
            p, t = t, xx * t - p
            buf[g, rows, :] = t.astype(jnp.bfloat16)
        prev[rows, :] = p
        cur[rows, :] = t

    def half_step(gen, use, level0):
        done = 0
        for g in range(GROUP):
            upto = (g + 1) * n_strips // GROUP
            for s in range(done, upto):
                gen_strip(gen, s)
            done = upto
            image = jnp.dot(lhs[...], use[g], preferred_element_type=jnp.float32)
            prod = image * fj[...]
            half_tile = TILE // 2
            acc[level0 + g] += prod[:, :half_tile] + prod[:, half_tile:]

    acc[...] = jnp.zeros_like(acc)
    fetch(0)
    begin(0)
    for s in range(n_strips):
        gen_strip(buf_a, s)

    def item_loop(item, carry):
        fetch(item + 1)
        set_operands(item)

        def chunk_loop(cp, carry):
            half_step(buf_b, buf_a, cp * 2 * GROUP)

            @pl.when(cp == CHUNKS // 2 - 1)
            def _():
                begin(item + 1)

            half_step(buf_a, buf_b, cp * 2 * GROUP + GROUP)
            return carry

        return lax.fori_loop(0, CHUNKS // 2, chunk_loop, carry)

    lax.fori_loop(0, n_items, item_loop, 0)
    out[...] = jnp.sum(acc[...], axis=-1)


def spectra_moments(cosines, ft, fct):
    maps = ft.shape[0]
    n = cosines.shape[1] // TILE
    table, counts, stride = work_tables(n)
    vmem = pl.BlockSpec(memory_space=pltpu.VMEM)
    smem = pl.BlockSpec(memory_space=pltpu.SMEM)
    return pl.pallas_call(
        functools.partial(moments_kernel, stride),
        out_shape=jax.ShapeDtypeStruct((LEVELS, maps), jnp.float32),
        in_specs=[smem, smem, pl.BlockSpec(memory_space=pl.ANY), vmem, vmem],
        out_specs=vmem,
        scratch_shapes=[
            pltpu.VMEM((2 * TILE, TILE), jnp.float32),
            pltpu.VMEM((2 * TILE, TILE), jnp.float32),
            pltpu.VMEM((2 * TILE, TILE), jnp.float32),
            pltpu.VMEM((2 * TILE, TILE), jnp.float32),
            pltpu.VMEM((GROUP, 2 * TILE, TILE), jnp.bfloat16),
            pltpu.VMEM((GROUP, 2 * TILE, TILE), jnp.bfloat16),
            pltpu.VMEM((maps, 2 * TILE), jnp.bfloat16),
            pltpu.VMEM((maps, TILE), jnp.float32),
            pltpu.VMEM((LEVELS, maps, TILE // 2), jnp.float32),
            pltpu.SemaphoreType.DMA((2,)),
        ],
        compiler_params=pltpu.CompilerParams(vmem_limit_bytes=48 * 2**20),
        name="moments",
    )(jnp.asarray(table), jnp.asarray(counts), cosines, ft, fct)


def per_device(npix, inverse_cov, cosines, sky_maps):
    cols_here = inverse_cov.shape[1]
    partial_value = jnp.dot(inverse_cov, sky_maps, preferred_element_type=jnp.float32)
    filtered = lax.psum(partial_value, "pcol").astype(jnp.bfloat16)
    column_index = lax.axis_index("pcol")
    full_maps = lax.all_gather(filtered, "prow", axis=0, tiled=True)
    filtered_cols = lax.dynamic_slice_in_dim(full_maps, column_index * cols_here, cols_here, 0)
    moments = spectra_moments(cosines, filtered.T, filtered_cols.T)
    row_sum = jnp.sum(filtered.astype(jnp.float32), axis=0)
    col_sum = jnp.sum(filtered_cols.astype(jnp.float32), axis=0)
    moments = jnp.concatenate([moments, (row_sum * col_sum)[None]], axis=0)
    matrix = jnp.asarray(transform_matrix(npix))
    partial_spectra = jnp.dot(matrix, moments, precision=lax.Precision.HIGHEST)
    spectra = lax.psum(partial_spectra, ("prow", "pcol"))
    return (filtered, spectra)


def solution(mesh):
    in_specs = (P("prow", "pcol"), P("prow", "pcol"), P("pcol", None))
    out_specs = (P("prow", None), P())

    def whole(inverse_cov, cosines, sky_maps):
        npix = cosines.shape[0]
        step = jax.shard_map(
            functools.partial(per_device, npix),
            mesh=mesh, in_specs=in_specs, out_specs=out_specs, check_vma=False,
        )
        return step(inverse_cov, cosines, sky_maps)

    return whole
```

```python
import functools
import math
import random

import jax
import jax.numpy as jnp
import numpy as np
from jax import lax
from jax.experimental import pallas as pl
from jax.experimental.pallas import tpu as pltpu
from jax.sharding import PartitionSpec as P

L = 64
LMIN = 2
TILE = 256
STRIP = 16
GROUP = 11
CHUNKS = 6
LEVELS = GROUP * CHUNKS


def transform_matrix(npix, devices):
    top = LMIN + L - 1
    each = -(-L // devices)
    a = [math.comb(2 * k, k) / 4.0**k for k in range(top + 1)]
    out = np.zeros((devices * 8, LEVELS))
    for l in range(LMIN, top + 1):
        owner, place = divmod(l - LMIN, each)
        row = out[owner * 8 + place]
        for k in range(l + 1):
            row[abs(l - 2 * k)] += a[k] * a[l - k]
        row *= (2 * l + 1) / npix
    return out.astype(np.float32), each


def pair_up(tiles, n):
    items = []
    for col in range(n):
        mine = sorted((t for t in tiles if t[1] == col), key=lambda t: t[0])
        for k in range(0, len(mine), 2):
            first = mine[k]
            second = mine[k + 1] if k + 1 < len(mine) else (first[0], col, 0)
            items.append((first[0], second[0], first[2], second[2], col))
    return items


def work_tables(n):
    lower = [[(h * n + i, j, 2) for i in range(n) for j in range(n)] for h in range(2)]
    rng = random.Random(0)
    best = None
    for _ in range(20000):
        sets = []
        cross = [[rng.random() < 0.5 for _ in range(n)] for _ in range(n)]
        for h in range(2):
            tiles = []
            for i in range(n):
                tiles.append((h * n + i, i, 1))
                for j in range(i):
                    a, b = (i, j) if rng.random() < 0.5 else (j, i)
                    tiles.append((h * n + a, b, 2))
                for j in range(n):
                    if h == 0 and cross[i][j]:
                        tiles.append((n + i, j, 2))
                    if h == 1 and not cross[i][j]:
                        tiles.append((j, i, 2))
            sets.append(pair_up(tiles, n))
        cost = max(len(s) for s in sets)
        if best is None or cost < best[0]:
            best = (cost, sets)
        if 2 * cost <= n * n + n // 2 + 1:
            break
    kinds = [pair_up(lower[0], n), pair_up(lower[1], n), pair_up(lower[1], n), pair_up(lower[0], n)] + best[1]
    longest = max(len(k) for k in kinds)
    table = np.zeros((len(kinds), longest + 1, 5), np.int32)
    for k, items in enumerate(kinds):
        table[k, : len(items)] = items
    counts = np.array([len(k) for k in kinds], np.int32)
    return table.reshape(-1), counts, longest + 1


def moments_kernel(
    stride, table, counts, cos_hbm, ft, fct, out,
    xbuf, x2, prev, cur, buf_a, buf_b, lhs, fj, acc, sem,
):
    r = lax.axis_index("prow")
    c = lax.axis_index("pcol")
    q, h = c // 2, c % 2
    kind = jnp.where(r > q, h, jnp.where(r < q, 2 + h, 4 + h))
    n_items = counts[kind]

    def field(item, f):
        return table[(kind * stride + item) * 5 + f]

    def tile_copy(item, half):
        row = pl.multiple_of(field(item, half) * TILE, TILE)
        col = pl.multiple_of(field(item, 4) * TILE, TILE)
        return pltpu.make_async_copy(
            cos_hbm.at[pl.ds(row, TILE), pl.ds(col, TILE)],
            xbuf.at[pl.ds(half * TILE, TILE)],
            sem.at[half],
        )

    def fetch(item):
        tile_copy(item, 0).start()
        tile_copy(item, 1).start()

    def begin(item):
        tile_copy(item, 0).wait()
        tile_copy(item, 1).wait()
        x = xbuf[...]
        x2[...] = x + x
        prev[...] = (x + x) * x - 1.0
        cur[...] = x

    def set_operands(item):
        col = pl.multiple_of(field(item, 4) * TILE, TILE)
        for half in range(2):
            row = pl.multiple_of(field(item, half) * TILE, TILE)
            weight = field(item, 2 + half).astype(jnp.float32)
            value = ft[:, pl.ds(row, TILE)].astype(jnp.float32) * weight
            lhs[:, half * TILE : (half + 1) * TILE] = value.astype(jnp.bfloat16)
        fj[...] = fct[:, pl.ds(col, TILE)].astype(jnp.float32)

    n_strips = 2 * TILE // STRIP

    def gen_strip(buf, s):
        rows = pl.ds(s * STRIP, STRIP)
        xx = x2[rows, :]
        p = prev[rows, :]
        t = cur[rows, :]
        for g in range(GROUP):
            p, t = t, xx * t - p
            buf[g, rows, :] = t.astype(jnp.bfloat16)
        prev[rows, :] = p
        cur[rows, :] = t

    def half_step(gen, use, level0):
        done = 0
        for g in range(GROUP):
            upto = (g + 1) * n_strips // GROUP
            for s in range(done, upto):
                gen_strip(gen, s)
            done = upto
            image = jnp.dot(lhs[...], use[g], preferred_element_type=jnp.float32)
            prod = image * fj[...]
            half_tile = TILE // 2
            acc[level0 + g] += prod[:, :half_tile] + prod[:, half_tile:]

    acc[...] = jnp.zeros_like(acc)
    fetch(0)
    begin(0)
    for s in range(n_strips):
        gen_strip(buf_a, s)

    def item_loop(item, carry):
        fetch(item + 1)
        set_operands(item)

        def chunk_loop(cp, carry):
            half_step(buf_b, buf_a, cp * 2 * GROUP)

            @pl.when(cp == CHUNKS // 2 - 1)
            def _():
                begin(item + 1)

            half_step(buf_a, buf_b, cp * 2 * GROUP + GROUP)
            return carry

        return lax.fori_loop(0, CHUNKS // 2, chunk_loop, carry)

    lax.fori_loop(0, n_items, item_loop, 0)
    out[...] = jnp.sum(acc[...], axis=-1)


def spectra_moments(cosines, ft, fct):
    maps = ft.shape[0]
    n = cosines.shape[1] // TILE
    table, counts, stride = work_tables(n)
    vmem = pl.BlockSpec(memory_space=pltpu.VMEM)
    smem = pl.BlockSpec(memory_space=pltpu.SMEM)
    return pl.pallas_call(
        functools.partial(moments_kernel, stride),
        out_shape=jax.ShapeDtypeStruct((LEVELS, maps), jnp.float32),
        in_specs=[smem, smem, pl.BlockSpec(memory_space=pl.ANY), vmem, vmem],
        out_specs=vmem,
        scratch_shapes=[
            pltpu.VMEM((2 * TILE, TILE), jnp.float32),
            pltpu.VMEM((2 * TILE, TILE), jnp.float32),
            pltpu.VMEM((2 * TILE, TILE), jnp.float32),
            pltpu.VMEM((2 * TILE, TILE), jnp.float32),
            pltpu.VMEM((GROUP, 2 * TILE, TILE), jnp.bfloat16),
            pltpu.VMEM((GROUP, 2 * TILE, TILE), jnp.bfloat16),
            pltpu.VMEM((maps, 2 * TILE), jnp.bfloat16),
            pltpu.VMEM((maps, TILE), jnp.float32),
            pltpu.VMEM((LEVELS, maps, TILE // 2), jnp.float32),
            pltpu.SemaphoreType.DMA((2,)),
        ],
        compiler_params=pltpu.CompilerParams(vmem_limit_bytes=48 * 2**20),
        name="moments",
    )(jnp.asarray(table), jnp.asarray(counts), cosines, ft, fct)


MESH = pl.DeviceIdType.MESH


def spread_kernel(n_q, block, out, far_send, near_send, far_recv, side_send, side_recv):
    r = lax.axis_index("prow")
    c = lax.axis_index("pcol")
    q, h = c // 2, c % 2
    width = block.shape[1]
    pieces = far_recv.shape[0]
    step = width // pieces
    partner = (r, c + 1 - 2 * h)
    above, below = (r, c + 2), (r, c - 2)
    has_above, has_below = q < n_q - 1, q > 0
    barrier = pltpu.get_barrier_semaphore()
    pl.semaphore_signal(barrier, inc=1, device_id=partner, device_id_type=MESH)

    @pl.when(has_above)
    def _():
        pl.semaphore_signal(barrier, inc=1, device_id=above, device_id_type=MESH)

    @pl.when(has_below)
    def _():
        pl.semaphore_signal(barrier, inc=1, device_id=below, device_id_type=MESH)

    pl.semaphore_wait(barrier, 1 + has_above.astype(jnp.int32) + has_below.astype(jnp.int32))

    source = q == r
    up = jnp.logical_and(q >= r, has_above)
    down = jnp.logical_and(q <= r, has_below)

    def columns(half, k):
        return pl.ds(pl.multiple_of(half * width + k * step, 128), step)

    def remote(src, k, send, recv, device):
        return pltpu.make_async_remote_copy(
            src_ref=src,
            dst_ref=out.at[:, columns(h, k)],
            send_sem=send.at[k],
            recv_sem=recv.at[k],
            device_id=device,
            device_id_type=MESH,
        )

    def send_all(src, k):
        @pl.when(up)
        def _():
            remote(src, k, far_send, far_recv, above).start()

        @pl.when(down)
        def _():
            remote(src, k, near_send, far_recv, below).start()

        remote(src, k, side_send, side_recv, partner).start()

    @pl.when(source)
    def _():
        for k in range(pieces):
            send_all(block.at[:, pl.ds(k * step, step)], k)
        out[:, pl.ds(pl.multiple_of(h * width, 128), width)] = block[...]

    @pl.when(jnp.logical_not(source))
    def _():
        for k in range(pieces):
            landed = out.at[:, columns(h, k)]
            remote(landed, k, side_send, far_recv, partner).wait_recv()
            send_all(landed, k)

    for k in range(pieces):
        mine = block.at[:, pl.ds(k * step, step)]

        @pl.when(up)
        def _():
            remote(mine, k, far_send, far_recv, above).wait_send()

        @pl.when(down)
        def _():
            remote(mine, k, near_send, far_recv, below).wait_send()

        remote(mine, k, side_send, side_recv, partner).wait_send()
        pltpu.make_async_remote_copy(
            src_ref=mine,
            dst_ref=out.at[:, columns(1 - h, k)],
            send_sem=side_send.at[k],
            recv_sem=side_recv.at[k],
            device_id=partner,
            device_id_type=MESH,
        ).wait_recv()


def spread(block, n_q, collective_id):
    maps, width = block.shape
    pieces = min(4, width // 128)
    vmem = pl.BlockSpec(memory_space=pltpu.VMEM)
    sems = pltpu.SemaphoreType.DMA((pieces,))
    return pl.pallas_call(
        functools.partial(spread_kernel, n_q),
        out_shape=jax.ShapeDtypeStruct((maps, 2 * width), block.dtype),
        in_specs=[vmem],
        out_specs=vmem,
        scratch_shapes=[sems] * 5,
        compiler_params=pltpu.CompilerParams(
            collective_id=collective_id, has_side_effects=True
        ),
        name="spread%d" % collective_id,
    )(block)


def sum_kernel(n, place_of, device_of, x, out, landed, result, send1, recv1, send2, recv2):
    me = place_of()
    barrier = pltpu.get_barrier_semaphore()

    def each(body):
        lax.fori_loop(1, n, lambda k, carry: (body(k), carry)[1], 0)

    def member(k):
        return device_of(lax.rem(me + k, n))

    each(lambda k: pl.semaphore_signal(barrier, inc=1, device_id=member(k), device_id_type=MESH))
    pl.semaphore_wait(barrier, n - 1)

    def scatter(k):
        return pltpu.make_async_remote_copy(
            src_ref=x.at[lax.rem(me + k, n)],
            dst_ref=landed.at[k - 1],
            send_sem=send1.at[k - 1],
            recv_sem=recv1.at[k - 1],
            device_id=member(k),
            device_id_type=MESH,
        )

    def gather(k, slot):
        return pltpu.make_async_remote_copy(
            src_ref=result,
            dst_ref=out.at[slot],
            send_sem=send2.at[k - 1],
            recv_sem=recv2.at[k - 1],
            device_id=member(k),
            device_id_type=MESH,
        )

    each(lambda k: scatter(k).start())
    each(lambda k: scatter(k).wait_recv())
    total = lax.fori_loop(0, n - 1, lambda k, t: t + landed[k], x[me]) if n > 8 else sum(
        (landed[k] for k in range(n - 1)), x[me]
    )
    result[...] = total.astype(result.dtype)
    each(lambda k: gather(k, me).start())
    out[me] = result[...]
    each(lambda k: gather(k, lax.rem(me - k + n, n)).wait_recv())
    each(lambda k: scatter(k).wait_send())
    each(lambda k: gather(k, me).wait_send())


def sum_and_share(x, dtype, place_of, device_of, collective_id):
    n, rows, cols = x.shape
    vmem = pl.BlockSpec(memory_space=pltpu.VMEM)
    sems = pltpu.SemaphoreType.DMA((n - 1,))
    return pl.pallas_call(
        functools.partial(sum_kernel, n, place_of, device_of),
        out_shape=jax.ShapeDtypeStruct(x.shape, dtype),
        in_specs=[vmem],
        out_specs=vmem,
        scratch_shapes=[
            pltpu.VMEM((n - 1, rows, cols), x.dtype),
            pltpu.VMEM((rows, cols), dtype),
            sems, sems, sems, sems,
        ],
        compiler_params=pltpu.CompilerParams(
            collective_id=collective_id, has_side_effects=True
        ),
        name="sum%d" % collective_id,
    )(x)


def per_device(npix, n_rows, n_cols, inverse_cov, cosines, sky_maps):
    maps = sky_maps.shape[1]
    cols_here = inverse_cov.shape[1]
    n_q = n_cols // 2
    sky_rows = spread(sky_maps.T, n_q, 1)
    partial_value = jnp.dot(sky_rows, inverse_cov, preferred_element_type=jnp.float32)
    column_maps = sum_and_share(
        partial_value.reshape(n_rows, maps // n_rows, cols_here),
        jnp.bfloat16,
        lambda: lax.axis_index("prow"),
        lambda i: (i, lax.axis_index("pcol")),
        2,
    ).reshape(maps, cols_here)
    row_maps = spread(column_maps, n_q, 3)
    moments = spectra_moments(cosines, row_maps, column_maps)
    devices = n_rows * n_cols
    matrix, each = transform_matrix(npix, devices)
    partial_spectra = jnp.dot(jnp.asarray(matrix), moments, precision=lax.Precision.HIGHEST)
    shared = sum_and_share(
        partial_spectra.reshape(devices, 8, maps),
        jnp.float32,
        lambda: lax.axis_index("prow") * n_cols + lax.axis_index("pcol"),
        lambda i: (i // n_cols, lax.rem(i, n_cols)),
        4,
    )
    spectra = shared[:, :each].reshape(devices * each, maps)[:L]
    return (row_maps.T, spectra)


def solution(mesh):
    in_specs = (P("prow", "pcol"), P("prow", "pcol"), P("pcol", None))
    out_specs = (P("prow", None), P())
    n_rows, n_cols = mesh.shape["prow"], mesh.shape["pcol"]

    def whole(inverse_cov, cosines, sky_maps):
        npix = cosines.shape[0]
        step = jax.shard_map(
            functools.partial(per_device, npix, n_rows, n_cols),
            mesh=mesh, in_specs=in_specs, out_specs=out_specs, check_vma=False,
        )
        return step(inverse_cov, cosines, sky_maps)

    return whole
```

```python
import functools
import math
import random

import jax
import jax.numpy as jnp
import numpy as np
from jax import lax
from jax.experimental import pallas as pl
from jax.experimental.pallas import tpu as pltpu
from jax.sharding import PartitionSpec as P

L = 64
LMIN = 2
TILE = 256
STRIP = 16
GROUP = 11
CHUNKS = 6
LEVELS = GROUP * CHUNKS


def transform_matrix(npix, devices):
    top = LMIN + L - 1
    each = -(-L // devices)
    a = [math.comb(2 * k, k) / 4.0**k for k in range(top + 1)]
    out = np.zeros((devices * each, LEVELS))
    for l in range(LMIN, top + 1):
        owner, place = divmod(l - LMIN, each)
        row = out[owner * each + place]
        for k in range(l + 1):
            row[abs(l - 2 * k)] += a[k] * a[l - k]
        row *= (2 * l + 1) / npix
    return out.astype(np.float32), each


def pair_up(tiles, n):
    items = []
    for col in range(n):
        mine = sorted((t for t in tiles if t[1] == col), key=lambda t: t[0])
        for k in range(0, len(mine), 2):
            first = mine[k]
            second = mine[k + 1] if k + 1 < len(mine) else (first[0], col, 0)
            items.append((first[0], second[0], first[2], second[2], col))
    return items


def work_tables(n):
    lower = [[(h * n + i, j, 2) for i in range(n) for j in range(n)] for h in range(2)]
    rng = random.Random(0)
    best = None
    for _ in range(20000):
        sets = []
        cross = [[rng.random() < 0.5 for _ in range(n)] for _ in range(n)]
        for h in range(2):
            tiles = []
            for i in range(n):
                tiles.append((h * n + i, i, 1))
                for j in range(i):
                    a, b = (i, j) if rng.random() < 0.5 else (j, i)
                    tiles.append((h * n + a, b, 2))
                for j in range(n):
                    if h == 0 and cross[i][j]:
                        tiles.append((n + i, j, 2))
                    if h == 1 and not cross[i][j]:
                        tiles.append((j, i, 2))
            sets.append(pair_up(tiles, n))
        cost = max(len(s) for s in sets)
        if best is None or cost < best[0]:
            best = (cost, sets)
        if 2 * cost <= n * n + n // 2 + 1:
            break
    kinds = [pair_up(lower[0], n), pair_up(lower[1], n), pair_up(lower[1], n), pair_up(lower[0], n)] + best[1]
    longest = max(len(k) for k in kinds)
    table = np.zeros((len(kinds), longest + 1, 5), np.int32)
    for k, items in enumerate(kinds):
        table[k, : len(items)] = items
    counts = np.array([len(k) for k in kinds], np.int32)
    return table.reshape(-1), counts, longest + 1


def moments_kernel(
    stride, table, counts, cos_hbm, ft, fct, out,
    xbuf, x2, prev, cur, buf_a, buf_b, lhs, fj, acc, sem,
):
    r = lax.axis_index("prow")
    c = lax.axis_index("pcol")
    q, h = c // 2, c % 2
    kind = jnp.where(r > q, h, jnp.where(r < q, 2 + h, 4 + h))
    n_items = counts[kind]

    def field(item, f):
        return table[(kind * stride + item) * 5 + f]

    def tile_copy(item, half):
        row = pl.multiple_of(field(item, half) * TILE, TILE)
        col = pl.multiple_of(field(item, 4) * TILE, TILE)
        return pltpu.make_async_copy(
            cos_hbm.at[pl.ds(row, TILE), pl.ds(col, TILE)],
            xbuf.at[pl.ds(half * TILE, TILE)],
            sem.at[half],
        )

    def fetch(item):
        tile_copy(item, 0).start()
        tile_copy(item, 1).start()

    def begin(item):
        tile_copy(item, 0).wait()
        tile_copy(item, 1).wait()
        x = xbuf[...]
        x2[...] = x + x
        prev[...] = (x + x) * x - 1.0
        cur[...] = x

    def set_operands(item):
        col = pl.multiple_of(field(item, 4) * TILE, TILE)
        for half in range(2):
            row = pl.multiple_of(field(item, half) * TILE, TILE)
            weight = field(item, 2 + half).astype(jnp.float32)
            value = ft[:, pl.ds(row, TILE)].astype(jnp.float32) * weight
            lhs[:, half * TILE : (half + 1) * TILE] = value.astype(jnp.bfloat16)
        fj[...] = fct[:, pl.ds(col, TILE)].astype(jnp.float32)

    n_strips = 2 * TILE // STRIP

    def gen_strip(buf, s):
        rows = pl.ds(s * STRIP, STRIP)
        xx = x2[rows, :]
        p = prev[rows, :]
        t = cur[rows, :]
        for g in range(GROUP):
            p, t = t, xx * t - p
            buf[g, rows, :] = t.astype(jnp.bfloat16)
        prev[rows, :] = p
        cur[rows, :] = t

    def half_step(gen, use, level0):
        done = 0
        for g in range(GROUP):
            upto = (g + 1) * n_strips // GROUP
            for s in range(done, upto):
                gen_strip(gen, s)
            done = upto
            image = jnp.dot(lhs[...], use[g], preferred_element_type=jnp.float32)
            prod = image * fj[...]
            half_tile = TILE // 2
            acc[level0 + g] += prod[:, :half_tile] + prod[:, half_tile:]

    acc[...] = jnp.zeros_like(acc)
    fetch(0)
    begin(0)
    for s in range(n_strips):
        gen_strip(buf_a, s)

    def item_loop(item, carry):
        fetch(item + 1)
        set_operands(item)

        def chunk_loop(cp, carry):
            half_step(buf_b, buf_a, cp * 2 * GROUP)

            @pl.when(cp == CHUNKS // 2 - 1)
            def _():
                begin(item + 1)

            half_step(buf_a, buf_b, cp * 2 * GROUP + GROUP)
            return carry

        return lax.fori_loop(0, CHUNKS // 2, chunk_loop, carry)

    lax.fori_loop(0, n_items, item_loop, 0)
    out[...] = jnp.sum(acc[...], axis=-1)


def spectra_moments(cosines, ft, fct):
    maps = ft.shape[0]
    n = cosines.shape[1] // TILE
    table, counts, stride = work_tables(n)
    vmem = pl.BlockSpec(memory_space=pltpu.VMEM)
    smem = pl.BlockSpec(memory_space=pltpu.SMEM)
    return pl.pallas_call(
        functools.partial(moments_kernel, stride),
        out_shape=jax.ShapeDtypeStruct((LEVELS, maps), jnp.float32),
        in_specs=[smem, smem, pl.BlockSpec(memory_space=pl.ANY), vmem, vmem],
        out_specs=vmem,
        scratch_shapes=[
            pltpu.VMEM((2 * TILE, TILE), jnp.float32),
            pltpu.VMEM((2 * TILE, TILE), jnp.float32),
            pltpu.VMEM((2 * TILE, TILE), jnp.float32),
            pltpu.VMEM((2 * TILE, TILE), jnp.float32),
            pltpu.VMEM((GROUP, 2 * TILE, TILE), jnp.bfloat16),
            pltpu.VMEM((GROUP, 2 * TILE, TILE), jnp.bfloat16),
            pltpu.VMEM((maps, 2 * TILE), jnp.bfloat16),
            pltpu.VMEM((maps, TILE), jnp.float32),
            pltpu.VMEM((LEVELS, maps, TILE // 2), jnp.float32),
            pltpu.SemaphoreType.DMA((2,)),
        ],
        compiler_params=pltpu.CompilerParams(vmem_limit_bytes=48 * 2**20),
        name="moments",
    )(jnp.asarray(table), jnp.asarray(counts), cosines, ft, fct)


MESH = pl.DeviceIdType.MESH


def spread_kernel(n_q, block, out, far_send, near_send, far_recv, side_send, side_recv):
    r = lax.axis_index("prow")
    c = lax.axis_index("pcol")
    q, h = c // 2, c % 2
    width = block.shape[1]
    pieces = far_recv.shape[0]
    step = width // pieces
    partner = (r, c + 1 - 2 * h)
    above, below = (r, c + 2), (r, c - 2)
    has_above, has_below = q < n_q - 1, q > 0
    barrier = pltpu.get_barrier_semaphore()
    pl.semaphore_signal(barrier, inc=1, device_id=partner, device_id_type=MESH)

    @pl.when(has_above)
    def _():
        pl.semaphore_signal(barrier, inc=1, device_id=above, device_id_type=MESH)

    @pl.when(has_below)
    def _():
        pl.semaphore_signal(barrier, inc=1, device_id=below, device_id_type=MESH)

    pl.semaphore_wait(barrier, 1 + has_above.astype(jnp.int32) + has_below.astype(jnp.int32))

    source = q == r
    up = jnp.logical_and(q >= r, has_above)
    down = jnp.logical_and(q <= r, has_below)

    def columns(half, k):
        return pl.ds(pl.multiple_of(half * width + k * step, 128), step)

    def remote(src, k, send, recv, device):
        return pltpu.make_async_remote_copy(
            src_ref=src,
            dst_ref=out.at[:, columns(h, k)],
            send_sem=send.at[k],
            recv_sem=recv.at[k],
            device_id=device,
            device_id_type=MESH,
        )

    def send_all(src, k):
        @pl.when(up)
        def _():
            remote(src, k, far_send, far_recv, above).start()

        @pl.when(down)
        def _():
            remote(src, k, near_send, far_recv, below).start()

        remote(src, k, side_send, side_recv, partner).start()

    @pl.when(source)
    def _():
        for k in range(pieces):
            send_all(block.at[:, pl.ds(k * step, step)], k)
        out[:, pl.ds(pl.multiple_of(h * width, 128), width)] = block[...]

    @pl.when(jnp.logical_not(source))
    def _():
        for k in range(pieces):
            landed = out.at[:, columns(h, k)]
            remote(landed, k, side_send, far_recv, partner).wait_recv()
            send_all(landed, k)

    for k in range(pieces):
        mine = block.at[:, pl.ds(k * step, step)]

        @pl.when(up)
        def _():
            remote(mine, k, far_send, far_recv, above).wait_send()

        @pl.when(down)
        def _():
            remote(mine, k, near_send, far_recv, below).wait_send()

        remote(mine, k, side_send, side_recv, partner).wait_send()
        pltpu.make_async_remote_copy(
            src_ref=mine,
            dst_ref=out.at[:, columns(1 - h, k)],
            send_sem=side_send.at[k],
            recv_sem=side_recv.at[k],
            device_id=partner,
            device_id_type=MESH,
        ).wait_recv()


def spread(block, n_q, collective_id):
    maps, width = block.shape
    pieces = width // 128
    vmem = pl.BlockSpec(memory_space=pltpu.VMEM)
    sems = pltpu.SemaphoreType.DMA((pieces,))
    return pl.pallas_call(
        functools.partial(spread_kernel, n_q),
        out_shape=jax.ShapeDtypeStruct((maps, 2 * width), block.dtype),
        in_specs=[vmem],
        out_specs=vmem,
        scratch_shapes=[sems] * 5,
        compiler_params=pltpu.CompilerParams(
            collective_id=collective_id, has_side_effects=True
        ),
        name="spread%d" % collective_id,
    )(block)


def sum_kernel(n, place_of, device_of, x, out, landed, result, send1, recv1, send2, recv2):
    me = place_of()
    barrier = pltpu.get_barrier_semaphore()

    def each(body):
        lax.fori_loop(1, n, lambda k, carry: (body(k), carry)[1], 0)

    def member(k):
        return device_of(lax.rem(me + k, n))

    each(lambda k: pl.semaphore_signal(barrier, inc=1, device_id=member(k), device_id_type=MESH))
    pl.semaphore_wait(barrier, n - 1)

    def scatter(k):
        return pltpu.make_async_remote_copy(
            src_ref=x.at[lax.rem(me + k, n)],
            dst_ref=landed.at[k - 1],
            send_sem=send1.at[k - 1],
            recv_sem=recv1.at[k - 1],
            device_id=member(k),
            device_id_type=MESH,
        )

    def gather(k, slot):
        return pltpu.make_async_remote_copy(
            src_ref=result,
            dst_ref=out.at[slot],
            send_sem=send2.at[k - 1],
            recv_sem=recv2.at[k - 1],
            device_id=member(k),
            device_id_type=MESH,
        )

    each(lambda k: scatter(k).start())
    each(lambda k: scatter(k).wait_recv())
    total = lax.fori_loop(0, n - 1, lambda k, t: t + landed[k], x[me]) if n > 8 else sum(
        (landed[k] for k in range(n - 1)), x[me]
    )
    result[...] = total.astype(result.dtype)
    each(lambda k: gather(k, me).start())
    out[me] = result[...]
    each(lambda k: gather(k, lax.rem(me - k + n, n)).wait_recv())
    each(lambda k: scatter(k).wait_send())
    each(lambda k: gather(k, me).wait_send())


def pair_kernel(
    n, place_of, device_of, x, out, from_pair, pair_sum, landed, result,
    send1, recv1, send2, recv2, send3, recv3, send4, recv4,
):
    me = place_of()
    m = n // 2
    side, spot = me % 2, me // 2
    partner = device_of(me + 1 - 2 * side)

    def member(k):
        return device_of(lax.rem(spot + k, m) * 2 + side)

    def copy(src, dst, send, recv, device):
        return pltpu.make_async_remote_copy(
            src_ref=src, dst_ref=dst, send_sem=send, recv_sem=recv,
            device_id=device, device_id_type=MESH,
        )

    def first(k):
        j = lax.rem(spot + k, m)
        return copy(x.at[2 * j + 1 - side], from_pair.at[j], send1.at[k - 1], recv1.at[k - 1], partner)

    def second(k):
        return copy(pair_sum.at[k - 1], landed.at[k - 1], send2.at[k - 1], recv2.at[k - 1], member(k))

    def third(k, slot):
        return copy(result, out.at[slot], send3.at[k - 1], recv3.at[k - 1], member(k))

    def fourth(k, parity):
        slot = lax.rem(spot - k + m, m) * 2 + parity
        src = result if k == 0 else out.at[slot]
        return copy(src, out.at[slot], send4.at[k], recv4.at[k], partner)

    barrier = pltpu.get_barrier_semaphore()
    pl.semaphore_signal(barrier, inc=1, device_id=partner, device_id_type=MESH)
    for k in range(1, m):
        pl.semaphore_signal(barrier, inc=1, device_id=member(k), device_id_type=MESH)
    pl.semaphore_wait(barrier, m)
    for k in range(1, m + 1):
        first(k).start()
    for k in range(1, m):
        j = lax.rem(spot + k, m)
        first(k).wait_recv()
        pair_sum[k - 1] = x[2 * j + side] + from_pair[j]
        second(k).start()
    first(m).wait_recv()
    total = x[me] + from_pair[spot]
    for k in range(1, m):
        second(k).wait_recv()
        total = total + landed[k - 1]
    result[...] = total.astype(result.dtype)
    for k in range(1, m):
        third(k, me).start()
    fourth(0, side).start()
    out[me] = result[...]
    for k in range(1, m):
        third(k, lax.rem(spot - k + m, m) * 2 + side).wait_recv()
        fourth(k, side).start()
    for k in range(m):
        fourth(k, 1 - side).wait_recv()
    for k in range(1, m + 1):
        first(k).wait_send()
    for k in range(1, m):
        second(k).wait_send()
        third(k, me).wait_send()
    for k in range(m):
        fourth(k, side).wait_send()


def pair_sum_and_share(x, dtype, place_of, device_of, collective_id):
    n, rows, cols = x.shape
    m = n // 2
    vmem = pl.BlockSpec(memory_space=pltpu.VMEM)
    whole, rest = pltpu.SemaphoreType.DMA((m,)), pltpu.SemaphoreType.DMA((m - 1,))
    return pl.pallas_call(
        functools.partial(pair_kernel, n, place_of, device_of),
        out_shape=jax.ShapeDtypeStruct(x.shape, dtype),
        in_specs=[vmem],
        out_specs=vmem,
        scratch_shapes=[
            pltpu.VMEM((m, rows, cols), x.dtype),
            pltpu.VMEM((m - 1, rows, cols), x.dtype),
            pltpu.VMEM((m - 1, rows, cols), x.dtype),
            pltpu.VMEM((rows, cols), dtype),
            whole, whole, rest, rest, rest, rest, whole, whole,
        ],
        compiler_params=pltpu.CompilerParams(
            collective_id=collective_id, has_side_effects=True
        ),
        name="sum%d" % collective_id,
    )(x)


def sum_and_share(x, dtype, place_of, device_of, collective_id):
    n, rows, cols = x.shape
    vmem = pl.BlockSpec(memory_space=pltpu.VMEM)
    sems = pltpu.SemaphoreType.DMA((n - 1,))
    return pl.pallas_call(
        functools.partial(sum_kernel, n, place_of, device_of),
        out_shape=jax.ShapeDtypeStruct(x.shape, dtype),
        in_specs=[vmem],
        out_specs=vmem,
        scratch_shapes=[
            pltpu.VMEM((n - 1, rows, cols), x.dtype),
            pltpu.VMEM((rows, cols), dtype),
            sems, sems, sems, sems,
        ],
        compiler_params=pltpu.CompilerParams(
            collective_id=collective_id, has_side_effects=True
        ),
        name="sum%d" % collective_id,
    )(x)


def per_device(npix, n_rows, n_cols, inverse_cov, cosines, sky_maps):
    maps = sky_maps.shape[1]
    cols_here = inverse_cov.shape[1]
    n_q = n_cols // 2
    sky_rows = spread(sky_maps.T, n_q, 1)
    partial_value = jnp.dot(sky_rows, inverse_cov, preferred_element_type=jnp.float32)
    column_maps = pair_sum_and_share(
        partial_value.reshape(n_rows, maps // n_rows, cols_here),
        jnp.bfloat16,
        lambda: lax.axis_index("prow"),
        lambda i: (i, lax.axis_index("pcol")),
        2,
    ).reshape(maps, cols_here)
    row_maps = spread(column_maps, n_q, 3)
    moments = spectra_moments(cosines, row_maps, column_maps)
    devices = n_rows * n_cols
    matrix, each = transform_matrix(npix, devices)
    partial_spectra = jnp.dot(jnp.asarray(matrix), moments, precision=lax.Precision.HIGHEST)
    shared = sum_and_share(
        partial_spectra.reshape(devices, each, maps),
        jnp.float32,
        lambda: lax.axis_index("prow") * n_cols + lax.axis_index("pcol"),
        lambda i: (i // n_cols, lax.rem(i, n_cols)),
        4,
    )
    spectra = shared.reshape(devices * each, maps)[:L]
    return (row_maps.T, spectra)


def solution(mesh):
    in_specs = (P("prow", "pcol"), P("prow", "pcol"), P("pcol", None))
    out_specs = (P("prow", None), P())
    n_rows, n_cols = mesh.shape["prow"], mesh.shape["pcol"]

    def whole(inverse_cov, cosines, sky_maps):
        npix = cosines.shape[0]
        step = jax.shard_map(
            functools.partial(per_device, npix, n_rows, n_cols),
            mesh=mesh, in_specs=in_specs, out_specs=out_specs, check_vma=False,
        )
        return step(inverse_cov, cosines, sky_maps)

    return whole
```
